512 devices in a mesh: space: 64 (over y_lo, z, x), tensor: 8 (over y_hi, core).
Axes of the slice: x: 4, y: 8 (y_hi: 4, y_lo: 2; y = y_hi * 2 + y_lo), z: 8, core: 2. Of those that a mesh axis runs over, the one named last changes fastest.
Arguments:
- tokens: float32 [2, 128, 128, 2048], P(None, 'space', None, 'tensor'), may hold values from -6 to 6
- in_gain: float32 [2048], replicated, may hold values from 0.25 to 1.75
- w_inner: bfloat16 [2048, 3072], P(None, 'tensor'), may hold values from -0.125 to 0.125
- w_bc: bfloat16 [2048, 256], replicated, may hold values from -0.03125 to 0.03125
- w_step: bfloat16 [2048, 48], P(None, 'tensor'), may hold values from -0.125 to 0.125
- step_bias: float32 [48], P('tensor'), may hold values from -3 to 0
- decay_rate: float32 [48], P('tensor'), may hold values from 0.02 to 2
- skip: float32 [48], P('tensor'), may hold values from 0.5 to 2
- norm_gain: float32 [3072], P('tensor'), may hold values from 0.25 to 1.75
- w_out: bfloat16 [3072, 2048], P('tensor'), may hold values from -0.109375 to 0.109375
Outputs:
- mixed: bfloat16 [2, 128, 128, 2048], P(None, 'space', None, 'tensor')
The draws below stay inside these ranges and needn't reach their ends.
All inputs are finite; a program needn't handle non-finite values.
Results may differ from the reference program's by a relative error of at most 0.011.
Values may be sent and summed in bfloat16 or wider, within the bound.
No kernel may reach another device: no remote copies, remote signals or barrier semaphores. Data moves between devices by JAX's collectives and lax.ppermute only.
A program may use at most 64 MiB of HBM per device.

```python
import math
import jax
import jax.numpy as jnp
from jax import lax

D = 2048
HEADS = 48
HEAD_DIM = 64
STATE = 128
NORM_HEADS = 6
H = 128
W = 128
IMAGES = 2
INNER = 3072


def shard_levels(own_key, shape, cuts, smallest, high):
    def one(dim, shards_of):
        heights = jax.random.uniform(jax.random.fold_in(jax.random.fold_in(own_key, 6), dim), (shards_of,), jnp.float32, smallest / len(cuts), high / len(cuts))
        return jnp.repeat(jnp.exp(heights), shape[dim] // shards_of).reshape((-1,) + (1,) * (len(shape) - dim - 1))

    loudness = one(*cuts[0])
    for cut in cuts[1:]:
        loudness = loudness * one(*cut)
    return loudness


def noise(stream_key, shape, spread, reach, shards=(), dtype=jnp.bfloat16):
    level = shard_levels(stream_key, shape, shards, -0.22, 0.18) if shards else 1.0
    entries = jax.random.normal(stream_key, shape, jnp.float32) * spread * level
    return jnp.minimum(jnp.maximum(entries, -reach), reach).astype(dtype)


def setup_inputs(seed: int = 0) -> dict:
    arg_keys = jax.random.split(jax.random.key(seed), 11)
    tokens = noise(arg_keys[0], (IMAGES, H, W, D), 1.0, 6.0, ((1, 64), (3, 8)), jnp.float32)
    in_gain = jnp.clip(1.0 + 0.15 * jax.random.normal(arg_keys[1], (D,), jnp.float32), 0.25, 1.75)
    w_inner = noise(arg_keys[2], (D, INNER), D ** -0.5, 0.125, ((1, 8),))
    w_bc = noise(arg_keys[3], (D, 2 * STATE), (D * 16) ** -0.5, 0.03125)
    w_step = noise(arg_keys[4], (D, HEADS), D ** -0.5, 0.125, ((1, 8),))
    step_bias = jnp.clip(-3.0 + 3.0 * jax.random.uniform(arg_keys[5], (HEADS,), jnp.float32) ** shard_levels(arg_keys[5], (HEADS,), ((0, 8),), -0.2, 0.2), -3.0, 0.0)
    decay_rate = jnp.clip(jnp.exp(math.log(2.0) - 4.6051702 * jax.random.uniform(arg_keys[6], (HEADS,), jnp.float32) ** shard_levels(arg_keys[6], (HEADS,), ((0, 8),), -0.2, 0.2)), 0.02, 2.0)
    skip = jnp.clip(0.5 + 1.5 * jax.random.uniform(arg_keys[7], (HEADS,), jnp.float32) ** shard_levels(arg_keys[7], (HEADS,), ((0, 8),), -0.2, 0.2), 0.5, 2.0)
    norm_gain = jnp.clip(1.0 + 0.15 * jax.random.normal(arg_keys[8], (INNER,), jnp.float32), 0.25, 1.75)
    w_out = noise(arg_keys[9], (INNER, D), INNER ** -0.5, 0.109375, ((0, 8),))
    return {"tokens": tokens, "in_gain": in_gain, "w_inner": w_inner, "w_bc": w_bc, "w_step": w_step, "step_bias": step_bias, "decay_rate": decay_rate, "skip": skip, "norm_gain": norm_gain, "w_out": w_out}


EPS = 1e-05

def kernel(logdecay):
    running = jnp.cumsum(logdecay, axis=-1)
    length = logdecay.shape[-1]
    place = jnp.arange(length)
    lower = place[:, None] >= place[None, :]
    upper = place[:, None] <= place[None, :]
    later = running[..., :, None] - running[..., None, :]
    shifted = running - logdecay
    earlier = shifted[..., None, :] - shifted[..., :, None]
    forward = jnp.exp(jnp.where(lower, later, -jnp.inf))
    backward = jnp.exp(jnp.where(upper, earlier, -jnp.inf))
    return forward + backward

def bidirectional(values, maps, logdecay):
    seqs, length, channels = values.shape
    heads = logdecay.shape[-1]
    in_map = maps[:, :, :STATE].astype(jnp.float32)
    out_map = maps[:, :, STATE:].astype(jnp.float32)
    scores = jnp.einsum('sln,smn->slm', out_map, in_map)
    split_values = values.reshape(seqs, length, heads, HEAD_DIM)
    decays = logdecay.astype(jnp.float32)

    def one_head(head):
        weights = (scores * kernel(decays[:, :, head])).astype(jnp.bfloat16)
        return jnp.einsum('slm,smp->slp', weights.astype(jnp.float32), split_values[:, :, head].astype(jnp.float32))
    outs = lax.map(one_head, jnp.arange(heads))
    return jnp.transpose(outs, (1, 2, 0, 3)).reshape(seqs, length, channels)

def reference(tokens, in_gain, w_inner, w_bc, w_step, step_bias, decay_rate, skip, norm_gain, w_out):
    rounded = tokens.astype(jnp.bfloat16).astype(jnp.float32)
    scale = lax.rsqrt(lax.optimization_barrier(jnp.mean(rounded * rounded, axis=-1, keepdims=True)) + EPS)
    normed = (rounded * scale * in_gain).astype(jnp.bfloat16)
    flat = normed.reshape(-1, D)
    inner = jnp.dot(flat, w_inner, preferred_element_type=jnp.float32).astype(jnp.bfloat16)
    maps = jnp.dot(flat, w_bc, preferred_element_type=jnp.float32).astype(jnp.bfloat16)
    step = jax.nn.softplus(jnp.dot(flat, w_step, preferred_element_type=jnp.float32) + step_bias)
    logdecay = (-decay_rate * step).astype(jnp.bfloat16)
    value = (inner.reshape(-1, HEADS, HEAD_DIM).astype(jnp.float32) * step[:, :, None]).reshape(-1, INNER).astype(jnp.bfloat16)
    value = value.reshape(IMAGES, H, W, INNER)
    maps = maps.reshape(IMAGES, H, W, 2 * STATE)
    logdecay = logdecay.reshape(IMAGES, H, W, HEADS)
    row_out = bidirectional(value.reshape(IMAGES * H, W, INNER), maps.reshape(IMAGES * H, W, 2 * STATE), logdecay.reshape(IMAGES * H, W, HEADS)).reshape(IMAGES, H, W, INNER)
    col_value = jnp.transpose(value, (0, 2, 1, 3)).reshape(IMAGES * W, H, INNER)
    col_maps = jnp.transpose(maps, (0, 2, 1, 3)).reshape(IMAGES * W, H, 2 * STATE)
    col_decay = jnp.transpose(logdecay, (0, 2, 1, 3)).reshape(IMAGES * W, H, HEADS)
    column_out = bidirectional(col_value, col_maps, col_decay).reshape(IMAGES, W, H, INNER)
    column_out = jnp.transpose(column_out, (0, 2, 1, 3)).astype(jnp.bfloat16)
    skip_wide = jnp.repeat(skip, HEAD_DIM)
    total = row_out + column_out.astype(jnp.float32) + skip_wide * inner.reshape(IMAGES, H, W, INNER).astype(jnp.float32)
    group = NORM_HEADS * HEAD_DIM
    grouped = total.reshape(IMAGES, H, W, INNER // group, group)
    norm_scale = lax.rsqrt(lax.optimization_barrier(jnp.mean(grouped * grouped, axis=-1, keepdims=True)) + EPS)
    gated = (grouped * norm_scale).reshape(IMAGES, H, W, INNER) * norm_gain
    gated = gated.astype(jnp.bfloat16)
    mixer = jnp.dot(gated.reshape(-1, INNER), w_out, preferred_element_type=jnp.float32).reshape(IMAGES, H, W, D)
    return (tokens + mixer).astype(jnp.bfloat16)
```

```python
import jax
import jax.numpy as jnp
from jax import lax
from jax.experimental import pallas as pl
from jax.experimental.pallas import tpu as pltpu
from jax.sharding import PartitionSpec as P

HEAD_DIM = 64
STATE = 128
LANES = 128
EPS = 1e-05
BF16 = jnp.bfloat16
F32 = jnp.float32


def dot(a, b, dims=((1,), (0,))):
    return lax.dot_general(a, b, (dims, ((), ())), preferred_element_type=F32)


def one_hot(rows, cols, target):
    t = lax.broadcasted_iota(jnp.int32, (rows, 1), 0)
    q = lax.broadcasted_iota(jnp.int32, (rows, cols), 1)
    return jnp.where(target(t) == q, 1.0, 0.0).astype(BF16)


def block(chip, core, part):
    chips = 4
    offset = (((chip + 2 * chips) & (chips - 1)) * 2 + core) * part
    return pl.ds(pl.multiple_of(offset, part), part)


def position():
    place = lax.axis_index("tensor")
    core = place & 1
    return place >> 1, core, 1 - 2 * core


def spots():
    y_hi, core, way = position()
    other = 1 - core
    early = [(y_hi, core), (y_hi - way, core), (y_hi + way, core)]
    early += [(y_hi, other), (y_hi + way, other), (y_hi - way, other)]
    return early, [(y_hi + 2, core), (y_hi + 2, other)]


def scaled(pieces, gain_ref, squares, y_ref):
    step_rows = 64
    part = pieces[0].shape[1]
    gains = [gain_ref[k : k + 1, :] for k in range(len(pieces))]

    def some(n, carry):
        rows = pl.ds(pl.multiple_of(n * step_rows, step_rows), step_rows)
        total = squares(rows)
        for k, ref in enumerate(pieces):
            x = ref[rows, :].astype(F32)
            y_ref[rows, k * part : (k + 1) * part] = (x * gains[k]).astype(BF16)
            x = x * x
            for m in range(part // LANES):
                total += x[:, m * LANES : (m + 1) * LANES]
        carry[rows, :] = total

    def loop(out_ref):
        @pl.loop(0, y_ref.shape[0] // step_rows)
        def _(n):
            some(n, out_ref)

    return loop


def prepare_kernel(*refs):
    gain_ref, w_inner_hbm, w_bc_hbm, w_step_ref, bias_ref, rate_ref = refs[:6]
    outs, small_ref, sems = (refs[6:9], refs[9:12]), refs[12], refs[13]
    channels, states = w_inner_hbm.shape[1], w_bc_hbm.shape[1]
    heads = w_step_ref.shape[0]
    part = outs[0][2].shape[1]
    copies = []
    for (w_ref, step_ref, gains_ref), blocks in zip(outs, spots()):
        for k, (chip, side) in enumerate(blocks):
            for source, lanes in ((w_inner_hbm, (0, channels)), (w_bc_hbm, (channels, states))):
                copy = pltpu.make_async_copy(
                    source.at[block(chip, side, part), :],
                    w_ref.at[pl.ds(k * part, part), pl.ds(*lanes)],
                    sems.at[len(copies)],
                )
                copy.start()
                copies.append(copy)
    small_ref[...] = jnp.zeros_like(small_ref)
    small_ref[0:1, :heads] = bias_ref[...]
    small_ref[1:2, :heads] = rate_ref[...]
    for (w_ref, step_ref, gains_ref), blocks in zip(outs, spots()):
        step_ref[...] = jnp.zeros_like(step_ref)
        gains_ref[...] = jnp.zeros_like(gains_ref)
        for k, (chip, side) in enumerate(blocks):
            step_ref[:heads, k * part : (k + 1) * part] = w_step_ref[:, block(chip, side, part)]
            row = ((chip + 8) & 3) * 4 + side * 2
            for m in range(part // LANES):
                gains_ref[k : k + 1, m * LANES : (m + 1) * LANES] = gain_ref[pl.ds(row + m, 1), :]
    for copy in copies:
        copy.wait()


def first_kernel(*refs):
    pieces = refs[:6]
    w_ref, step_ref, gain_ref = refs[6:9]
    acc_ref, squares_ref, y_ref = refs[9:]
    wide = w_ref.shape[1]
    scaled(pieces, gain_ref, lambda rows: jnp.zeros((64, LANES), F32), y_ref)(squares_ref)
    y = y_ref[...]
    acc_ref[:, :wide] = dot(y, w_ref[...])
    acc_ref[:, wide:] = dot(y, step_ref[...], ((1,), (1,)))


def project_kernel(*refs):
    pieces = refs[:2]
    w_ref, step_ref, gain_ref, small_ref, acc_ref, squares_ref = refs[2:8]
    send_ref, inner_ref, value_ref, side_ref = refs[8:12]
    y_ref, total_ref = refs[12:]
    patches = pieces[0].shape[0]
    channels = inner_ref.shape[1]
    wide = w_ref.shape[1]
    states = wide - channels
    scaled(pieces, gain_ref, lambda rows: squares_ref[rows, :], y_ref)(total_ref)
    mean = jnp.sum(total_ref[...], axis=-1, keepdims=True) / (4 * y_ref.shape[1])
    scale = lax.rsqrt(mean + EPS)
    y = y_ref[...]
    raw = acc_ref[:, wide:] + dot(y, step_ref[...], ((1,), (1,)))
    step = jax.nn.softplus(raw * scale + small_ref[0:1, :])
    side_ref[:, states:] = (-small_ref[1:2, :] * step).astype(BF16)
    maps = acc_ref[:, channels:wide] + dot(y, w_ref[:, channels:])
    side_ref[:, :states] = (maps * scale).astype(BF16)
    inner = ((acc_ref[:, :channels] + dot(y, w_ref[:, :channels])) * scale).astype(BF16)
    inner_ref[...] = inner
    left = lax.broadcasted_iota(jnp.int32, (patches, LANES), 1) < HEAD_DIM
    for k in range(channels // LANES):
        widened = jnp.where(left, step[:, 2 * k : 2 * k + 1], step[:, 2 * k + 1 : 2 * k + 2])
        at = slice(k * LANES, (k + 1) * LANES)
        value_ref[:, at] = (inner[:, at].astype(F32) * widened).astype(BF16)
    order = one_hot(patches, patches, lambda t: ((t & 3) << 7) + ((t >> 3) << 1) + ((t >> 2) & 1))
    send_ref[:, :channels] = dot(order, value_ref[...]).astype(BF16)
    send_ref[:, channels:] = dot(order, side_ref[...]).astype(BF16)


def scan(value, side):
    length = value.shape[0]
    heads = value.shape[1] // HEAD_DIM
    in_map, out_map = side[:, :STATE], side[:, STATE : 2 * STATE]
    decay = side[:, 2 * STATE :]
    scores = dot(out_map, in_map, ((1,), (1,)))
    t = lax.broadcasted_iota(jnp.int32, (length, length), 0)
    r = lax.broadcasted_iota(jnp.int32, (length, length), 1)
    lower = jnp.where(t >= r, 1.0, 0.0).astype(BF16)
    upper = jnp.where(t <= r, 1.0, 0.0).astype(BF16)
    unit = jnp.where(t == r, 1.0, 0.0).astype(BF16)
    running = dot(lower, decay)
    across = dot(decay, upper, ((0,), (0,)))
    shifted = running - decay.astype(F32)
    shifted_across = across - dot(decay, unit, ((0,), (0,)))
    doubled = jnp.where(t == r, 2.0 * scores, scores)
    below = r <= t
    outs = []
    for h in range(heads):
        later = running[:, h : h + 1] - across[h : h + 1, :]
        earlier = shifted_across[h : h + 1, :] - shifted[:, h : h + 1]
        weights = doubled * jnp.exp(jnp.where(below, jnp.where(t == r, 0.0, later), earlier))
        outs.append(
            dot(weights.astype(BF16), value[:, h * HEAD_DIM : (h + 1) * HEAD_DIM])
        )
    return jnp.concatenate(outs, axis=1)


def row_kernel(value_ref, side_ref, inner_ref, skip_ref, out_ref):
    length = LANES
    for row in range(value_ref.shape[0] // length):
        at = pl.ds(row * length, length)
        out_ref[at, :] = (
            scan(value_ref[at, :], side_ref[at, :])
            + skip_ref[...] * inner_ref[at, :].astype(F32)
        )


def column_kernel(recv_ref, back_ref, sorted_ref, outs_ref):
    rows = recv_ref.shape[0]
    channels = back_ref.shape[1]
    length = rows // 4
    order = one_hot(
        rows, rows, lambda t: (((t & 127) >> 1) << 3) + ((t >> 7) << 1) + (t & 1)
    )
    sorted_ref[...] = dot(order, recv_ref[...]).astype(BF16)
    for n in range(4):
        at = pl.ds(n * length, length)
        outs_ref[at, :] = scan(sorted_ref[at, :channels], sorted_ref[at, channels:]).astype(BF16)
    back = one_hot(rows, rows, lambda t: (((t >> 1) & 3) << 7) + ((t >> 3) << 1) + (t & 1))
    back_ref[...] = dot(back, outs_ref[...]).astype(BF16)


def output_kernel(back_ref, row_ref, gain_ref, w_ref, *out_refs):
    y_hi, core, way = position()
    patches = row_ref.shape[0]
    order = one_hot(
        patches, patches, lambda t: (((t & 127) >> 1) << 3) + ((t & 1) << 2) + (t >> 7)
    )
    total = row_ref[...] + dot(order, back_ref[...])
    scale = lax.rsqrt(jnp.mean(total * total, axis=-1, keepdims=True) + EPS)
    gated = (total * scale * gain_ref[...]).astype(BF16)
    part = out_refs[0].shape[1]
    spots = [(2, 1 - core), (way, 1 - core), (-way, 1 - core), (0, 1 - core)]
    spots += [(2, core), (-way, core), (way, core), (0, core)]
    for ref, (chip, side) in zip(out_refs, spots):
        ref[...] = dot(gated, w_ref[:, block(y_hi + chip, side, part)]).astype(ref.dtype)


def call(body, outs, args, flops, scratch=(), in_hbm=()):
    size = sum(a.size * a.dtype.itemsize for a in args)
    size += sum(o.size * o.dtype.itemsize for o in outs)
    return pl.pallas_call(
        body,
        out_shape=outs,
        in_specs=[
            pl.BlockSpec(memory_space=pltpu.HBM if n in in_hbm else pltpu.VMEM)
            for n in range(len(args))
        ],
        out_specs=[pl.BlockSpec(memory_space=pltpu.VMEM)] * len(outs),
        scratch_shapes=list(scratch),
        cost_estimate=pl.CostEstimate(flops=flops, bytes_accessed=size, transcendentals=0),
        compiler_params=pltpu.CompilerParams(vmem_limit_bytes=24 * 1024 * 1024),
    )(*args)


def shape(dims, dtype):
    return jax.ShapeDtypeStruct(dims, dtype)


def hop(x, sign):
    pairs = []
    for t in range(8):
        way = sign * (1 - 2 * (t & 1))
        pairs.append((t, (t + 2 * way) % 8))
    return lax.ppermute(x, "tensor", pairs)


def swap(x):
    return lax.ppermute(x, "tensor", [(t, t ^ 1) for t in range(8)])


def layer(
    tokens, in_gain, w_inner, w_bc, w_step, step_bias, decay_rate, skip, norm_gain, w_out
):
    images, rows, width, part = tokens.shape
    patches = images * rows * width
    channels = w_inner.shape[1]
    gain = in_gain.reshape(-1, LANES)
    bias = step_bias[None, :]
    rate = decay_rate[None, :]
    skip_wide = jnp.repeat(skip, HEAD_DIM)[None, :]
    out_gain = norm_gain[None, :]
    flat = tokens.reshape(patches, part)
    space = lax.axis_size("space")

    def exchange(x):
        y = x.reshape(space, -1, x.shape[-1])
        y = lax.all_to_all(y, "space", split_axis=0, concat_axis=0, tiled=True)
        return y.reshape(x.shape)

    x = flat.astype(BF16)
    ahead, behind = hop(x, 1), hop(x, -1)
    wide = channels + 2 * STATE
    counts = [6 * part, 2 * part]
    orders = [
        o
        for n in counts
        for o in (shape((n, wide), BF16), shape((LANES, n), BF16), shape((8, part), F32))
    ]
    prepared = call(
        prepare_kernel,
        orders + [shape((8, LANES), F32)],
        [gain, w_inner, w_bc, w_step.T, bias, rate],
        4 * 10**9,
        [pltpu.SemaphoreType.DMA((16,))],
        in_hbm=(1, 2),
    )
    ahead, *prepared = lax.optimization_barrier((ahead, *prepared))
    across = hop(ahead, 1)
    early = [x, ahead, behind, swap(x), swap(ahead), swap(behind)]
    started = call(
        first_kernel,
        [shape((patches, wide + LANES), F32), shape((patches, LANES), F32)],
        early + prepared[:3],
        4 * 10**9,
        [pltpu.VMEM((patches, counts[0]), BF16)],
    )
    across, *started = lax.optimization_barrier((across, *started))
    pieces = [across, swap(across)]
    wide += LANES
    dims = [(patches, wide), (patches, channels), (patches, channels), (patches, wide - channels)]
    send, inner, value, side = call(
        project_kernel,
        [shape(d, BF16) for d in dims],
        pieces + prepared[3:] + started,
        2 * 10**9,
        [pltpu.VMEM((patches, counts[1]), BF16), pltpu.VMEM((patches, LANES), F32)],
    )
    got = exchange(send)
    (back,) = call(
        column_kernel,
        [shape((patches, channels), BF16)],
        [got],
        8 * 10**8,
        [pltpu.VMEM((patches, wide), BF16), pltpu.VMEM((patches, channels), BF16)],
    )
    back = exchange(back)
    (row,) = call(
        row_kernel, [shape((patches, channels), F32)], [value, side, inner, skip_wide], 8 * 10**8
    )
    pieces = call(
        output_kernel,
        [shape((patches, part), BF16)] * 4 + [shape((patches, part), F32)] * 4,
        [back, row, out_gain, w_out],
        2 * patches * channels * 2048,
    )
    give, keep = pieces[:4], pieces[4:]
    taken = [swap(g).astype(F32) for g in give]
    sums = [k + t for k, t in zip(keep, taken)]
    far = hop(sums[0].astype(BF16), 1)
    near = hop(sums[1].astype(BF16), -1)
    last = hop((sums[2] + far.astype(F32)).astype(BF16), 1)
    total = flat + sums[3] + near.astype(F32) + last.astype(F32)
    return total.astype(BF16).reshape(tokens.shape)


def solution(mesh):
    return jax.shard_map(
        layer,
        mesh=mesh,
        in_specs=(
            P(None, "space", None, "tensor"),
            P(),
            P(None, "tensor"),
            P(),
            P(None, "tensor"),
            P("tensor"),
            P("tensor"),
            P("tensor"),
            P("tensor"),
            P("tensor", None),
        ),
        out_specs=P(None, "space", None, "tensor"),
        check_vma=False,
    )
```

```python
import jax
import jax.numpy as jnp
from jax import lax
from jax.experimental import pallas as pl
from jax.experimental.pallas import tpu as pltpu
from jax.sharding import PartitionSpec as P

HEAD_DIM = 64
STATE = 128
LANES = 128
EPS = 1e-05
BF16 = jnp.bfloat16
F32 = jnp.float32


def dot(a, b, dims=((1,), (0,))):
    return lax.dot_general(a, b, (dims, ((), ())), preferred_element_type=F32)


def one_hot(rows, cols, target):
    t = lax.broadcasted_iota(jnp.int32, (rows, 1), 0)
    q = lax.broadcasted_iota(jnp.int32, (rows, cols), 1)
    return jnp.where(target(t) == q, 1.0, 0.0).astype(BF16)


def block(chip, core, part):
    chips = 4
    offset = (((chip + 2 * chips) & (chips - 1)) * 2 + core) * part
    return pl.ds(pl.multiple_of(offset, part), part)


def position():
    place = lax.axis_index("tensor")
    core = place & 1
    return place >> 1, core, 1 - 2 * core


def spots():
    y_hi, core, way = position()
    other = 1 - core
    early = [(y_hi, core), (y_hi - way, core), (y_hi, other), (y_hi + way, other)]
    late = [(y_hi + way, core), (y_hi + 2, core), (y_hi - way, other), (y_hi + 2, other)]
    return early, late


def scaled(pieces, gain_ref, squares, y_ref, counted=0):
    step_rows = 64
    part = pieces[0].shape[1]
    gains = [gain_ref[k : k + 1, :] for k in range(len(pieces))]

    def some(n, carry):
        rows = pl.ds(pl.multiple_of(n * step_rows, step_rows), step_rows)
        total = squares(rows)
        for k, ref in enumerate(pieces):
            x = ref[rows, :].astype(F32)
            y_ref[rows, k * part : (k + 1) * part] = (x * gains[k]).astype(BF16)
            if k < counted:
                continue
            x = x * x
            for m in range(part // LANES):
                total += x[:, m * LANES : (m + 1) * LANES]
        carry[rows, :] = total

    def loop(out_ref):
        @pl.loop(0, y_ref.shape[0] // step_rows)
        def _(n):
            some(n, out_ref)

    return loop


def prepare_kernel(*refs):
    gain_ref, w_inner_hbm, w_bc_hbm, w_step_ref, bias_ref, rate_ref = refs[:6]
    outs, small_ref, sems = (refs[6:9], refs[9:12]), refs[12], refs[13]
    channels, states = w_inner_hbm.shape[1], w_bc_hbm.shape[1]
    heads = w_step_ref.shape[0]
    part = outs[0][2].shape[1]
    copies = []
    for (w_ref, step_ref, gains_ref), blocks in zip(outs, spots()):
        for k, (chip, side) in enumerate(blocks):
            for source, lanes in ((w_inner_hbm, (0, channels)), (w_bc_hbm, (channels, states))):
                copy = pltpu.make_async_copy(
                    source.at[block(chip, side, part), :],
                    w_ref.at[pl.ds(k * part, part), pl.ds(*lanes)],
                    sems.at[len(copies)],
                )
                copy.start()
                copies.append(copy)
    small_ref[...] = jnp.zeros_like(small_ref)
    small_ref[0:1, :heads] = bias_ref[...]
    small_ref[1:2, :heads] = rate_ref[...]
    for (w_ref, step_ref, gains_ref), blocks in zip(outs, spots()):
        step_ref[...] = jnp.zeros_like(step_ref)
        gains_ref[...] = jnp.zeros_like(gains_ref)
        for k, (chip, side) in enumerate(blocks):
            step_ref[:heads, k * part : (k + 1) * part] = w_step_ref[:, block(chip, side, part)]
            row = ((chip + 8) & 3) * 4 + side * 2
            for m in range(part // LANES):
                gains_ref[k : k + 1, m * LANES : (m + 1) * LANES] = gain_ref[pl.ds(row + m, 1), :]
    for copy in copies:
        copy.wait()


def squares_kernel(x_ref, squares_ref):
    x = x_ref[...].astype(F32)
    x = x * x
    squares_ref[...] = x[:, :LANES] + x[:, LANES:]


def first_kernel(*refs):
    pieces = refs[:4]
    w_ref, step_ref, gain_ref, begun_ref = refs[4:8]
    acc_ref, squares_ref, y_ref = refs[8:]
    wide = w_ref.shape[1]
    scaled(pieces, gain_ref, lambda rows: begun_ref[rows, :], y_ref, 1)(squares_ref)
    y = y_ref[...]
    acc_ref[:, :wide] = dot(y, w_ref[...])
    acc_ref[:, wide:] = dot(y, step_ref[...], ((1,), (1,)))


def gathered(x, b):
    return jnp.concatenate([x[n * 128 + b * 64 : n * 128 + b * 64 + 64] for n in range(4)], axis=0)


def project_kernel(*refs):
    pieces = refs[:4]
    w_ref, step_ref, gain_ref, small_ref, acc_ref, squares_ref = refs[4:10]
    send_ref, inner_ref, value_ref, side_ref = refs[10:14]
    y_ref, total_ref = refs[14:]
    patches = pieces[0].shape[0]
    channels = inner_ref.shape[1]
    wide = w_ref.shape[1]
    states = wide - channels
    scaled(pieces, gain_ref, lambda rows: squares_ref[rows, :], y_ref)(total_ref)
    mean = jnp.sum(total_ref[...], axis=-1, keepdims=True) / (2 * y_ref.shape[1])
    scale = lax.rsqrt(mean + EPS)
    y = y_ref[...]
    raw = acc_ref[:, wide:] + dot(y, step_ref[...], ((1,), (1,)))
    step = jax.nn.softplus(raw * scale + small_ref[0:1, :])
    side_ref[:, states:] = (-small_ref[1:2, :] * step).astype(BF16)
    maps = acc_ref[:, channels:wide] + dot(y, w_ref[:, channels:])
    side_ref[:, :states] = (maps * scale).astype(BF16)
    inner = ((acc_ref[:, :channels] + dot(y, w_ref[:, :channels])) * scale).astype(BF16)
    inner_ref[...] = inner
    left = lax.broadcasted_iota(jnp.int32, (patches, LANES), 1) < HEAD_DIM
    for k in range(channels // LANES):
        widened = jnp.where(left, step[:, 2 * k : 2 * k + 1], step[:, 2 * k + 1 : 2 * k + 2])
        at = slice(k * LANES, (k + 1) * LANES)
        value_ref[:, at] = (inner[:, at].astype(F32) * widened).astype(BF16)
    target = lambda t: ((t & 3) << 6) + ((t >> 3) << 1) + ((t >> 2) & 1)
    order = one_hot(256, 256, target)
    for b in range(patches // 256):
        rows = slice(b * 256, (b + 1) * 256)
        send_ref[rows, :channels] = dot(order, gathered(value_ref, b)).astype(BF16)
        send_ref[rows, channels:] = dot(order, gathered(side_ref, b)).astype(BF16)


def scan(value, side):
    length = value.shape[0]
    heads = value.shape[1] // HEAD_DIM
    in_map, out_map = side[:, :STATE], side[:, STATE : 2 * STATE]
    decay = side[:, 2 * STATE :]
    scores = dot(out_map, in_map, ((1,), (1,)))
    t = lax.broadcasted_iota(jnp.int32, (length, length), 0)
    r = lax.broadcasted_iota(jnp.int32, (length, length), 1)
    lower = jnp.where(t >= r, 1.0, 0.0).astype(BF16)
    upper = jnp.where(t <= r, 1.0, 0.0).astype(BF16)
    unit = jnp.where(t == r, 1.0, 0.0).astype(BF16)
    running = dot(lower, decay)
    across = dot(decay, upper, ((0,), (0,)))
    shifted = running - decay.astype(F32)
    shifted_across = across - dot(decay, unit, ((0,), (0,)))
    doubled = jnp.where(t == r, 2.0 * scores, scores)
    below = r < t
    left = lax.broadcasted_iota(jnp.int32, (length, LANES), 1) < HEAD_DIM

    def weights(h):
        later = running[:, h : h + 1] - across[h : h + 1, :]
        earlier = shifted_across[h : h + 1, :] - shifted[:, h : h + 1]
        exponent = jnp.where(t == r, 0.0, jnp.where(below, later, earlier))
        return (doubled * jnp.exp(exponent)).astype(BF16)

    outs = []
    for k in range(heads // 2):
        pair = value[:, k * LANES : (k + 1) * LANES]
        zero = jnp.zeros_like(pair)
        stacked = jnp.concatenate([jnp.where(left, pair, zero), jnp.where(left, zero, pair)], axis=0)
        both = jnp.concatenate([weights(2 * k), weights(2 * k + 1)], axis=1)
        outs.append(dot(both, stacked))
    return jnp.concatenate(outs, axis=1)


def row_kernel(value_ref, side_ref, inner_ref, skip_ref, out_ref):
    length = LANES
    for row in range(value_ref.shape[0] // length):
        at = pl.ds(row * length, length)
        out_ref[at, :] = (
            scan(value_ref[at, :], side_ref[at, :])
            + skip_ref[...] * inner_ref[at, :].astype(F32)
        )


def column_kernel(recv_ref, back_ref, sorted_ref, outs_ref):
    rows = recv_ref.shape[0]
    channels = back_ref.shape[1]
    length = rows // 4
    order = one_hot(256, 256, lambda t: (((t & 63) >> 1) << 3) + ((t >> 6) << 1) + (t & 1))
    for b in range(rows // 256):
        block_rows = dot(order, recv_ref[b * 256 : (b + 1) * 256, :]).astype(BF16)
        for n in range(4):
            sorted_ref[n * length + b * 64 : n * length + b * 64 + 64, :] = block_rows[n * 64 : n * 64 + 64]
    for n in range(4):
        at = pl.ds(n * length, length)
        outs_ref[at, :] = scan(sorted_ref[at, :channels], sorted_ref[at, channels:]).astype(BF16)
    back = one_hot(256, 256, lambda t: (((t >> 1) & 3) << 6) + ((t >> 3) << 1) + (t & 1))
    for b in range(rows // 256):
        back_ref[b * 256 : (b + 1) * 256, :] = dot(back, gathered(outs_ref, b)).astype(BF16)


def arrange_kernel(w_hbm, keep_ref, give_ref, sems):
    y_hi, core, way = position()
    part = keep_ref.shape[1] // 4
    copies = []
    for ref, side, toward in ((give_ref, 1 - core, -way), (keep_ref, core, way)):
        for k, chip in enumerate((2, -toward, toward, 0)):
            copy = pltpu.make_async_copy(
                w_hbm.at[:, block(y_hi + chip, side, part)],
                ref.at[:, pl.ds(k * part, part)],
                sems.at[len(copies)],
            )
            copy.start()
            copies.append(copy)
    for copy in copies:
        copy.wait()


def gate_kernel(back_ref, row_ref, gain_ref, gated_ref):
    order = one_hot(256, 256, lambda t: (((t & 63) >> 1) << 3) + ((t & 1) << 2) + (t >> 6))
    for b in range(row_ref.shape[0] // 256):
        total = gathered(row_ref, b) + dot(order, back_ref[b * 256 : (b + 1) * 256, :])
        scale = lax.rsqrt(jnp.mean(total * total, axis=-1, keepdims=True) + EPS)
        gated = (total * scale * gain_ref[...]).astype(BF16)
        for n in range(4):
            gated_ref[n * 128 + b * 64 : n * 128 + b * 64 + 64, :] = gated[n * 64 : n * 64 + 64]


def far_kernel(gated_ref, peer_ref, keep_ref, got_ref, far_ref):
    at = slice(0, far_ref.shape[1])
    far_ref[...] = (
        dot(gated_ref[...], keep_ref[:, at]) + dot(peer_ref[...], got_ref[:, at])
    ).astype(BF16)


def output_kernel(gated_ref, peer_ref, keep_ref, got_ref, tokens_ref, near_ref, last_ref, own_ref):
    part = near_ref.shape[1]
    gated, peer = gated_ref[...], peer_ref[...]
    for k, ref in enumerate((near_ref, last_ref, own_ref)):
        at = slice((k + 1) * part, (k + 2) * part)
        total = dot(gated, keep_ref[:, at]) + dot(peer, got_ref[:, at])
        if ref is own_ref:
            total += tokens_ref[...]
        ref[...] = total.astype(ref.dtype)


def call(body, outs, args, flops, scratch=(), in_hbm=()):
    size = sum(a.size * a.dtype.itemsize for a in args)
    size += sum(o.size * o.dtype.itemsize for o in outs)
    return pl.pallas_call(
        body,
        out_shape=outs,
        in_specs=[
            pl.BlockSpec(memory_space=pltpu.HBM if n in in_hbm else pltpu.VMEM)
            for n in range(len(args))
        ],
        out_specs=[pl.BlockSpec(memory_space=pltpu.VMEM)] * len(outs),
        scratch_shapes=list(scratch),
        cost_estimate=pl.CostEstimate(flops=flops, bytes_accessed=size, transcendentals=0),
        compiler_params=pltpu.CompilerParams(vmem_limit_bytes=24 * 1024 * 1024),
    )(*args)


def shape(dims, dtype):
    return jax.ShapeDtypeStruct(dims, dtype)


def hop(x, sign):
    pairs = []
    for t in range(8):
        way = sign * (1 - 2 * (t & 1))
        pairs.append((t, (t + 2 * way) % 8))
    return lax.ppermute(x, "tensor", pairs)


def swap(x):
    return lax.ppermute(x, "tensor", [(t, t ^ 1) for t in range(8)])


def layer(
    tokens, in_gain, w_inner, w_bc, w_step, step_bias, decay_rate, skip, norm_gain, w_out
):
    images, rows, width, part = tokens.shape
    patches = images * rows * width
    channels = w_inner.shape[1]
    gain = in_gain.reshape(-1, LANES)
    bias = step_bias[None, :]
    rate = decay_rate[None, :]
    skip_wide = jnp.repeat(skip, HEAD_DIM)[None, :]
    out_gain = norm_gain[None, :]
    flat = tokens.reshape(patches, part)
    space = lax.axis_size("space")

    def exchange(x):
        y = x.reshape(space, -1, x.shape[-1])
        y = lax.all_to_all(y, "space", split_axis=0, concat_axis=0, tiled=True)
        return y.reshape(x.shape)

    x = flat.astype(BF16)
    ahead, behind = hop(x, 1), hop(x, -1)
    wide = channels + 2 * STATE
    counts = [4 * part, 4 * part]
    orders = [
        o
        for n in counts
        for o in (shape((n, wide), BF16), shape((LANES, n), BF16), shape((8, part), F32))
    ]
    (begun,) = call(squares_kernel, [shape((patches, LANES), F32)], [x], 4 * 10**10)
    begun, *sources = lax.optimization_barrier((begun, gain, w_inner, w_bc, w_step.T, bias, rate))
    prepared = call(
        prepare_kernel,
        orders + [shape((8, LANES), F32)],
        sources,
        4 * 10**9,
        [pltpu.SemaphoreType.DMA((16,))],
        in_hbm=(1, 2),
    )
    ahead, *prepared = lax.optimization_barrier((ahead, *prepared))
    across = hop(ahead, 1)
    early = [x, ahead, swap(x), swap(ahead)]
    started = call(
        first_kernel,
        [shape((patches, wide + LANES), F32), shape((patches, LANES), F32)],
        early + prepared[:3] + [begun],
        4 * 10**9,
        [pltpu.VMEM((patches, counts[0]), BF16)],
    )
    behind, *started = lax.optimization_barrier((behind, *started))
    peer_behind = swap(behind)
    across, peer_behind = lax.optimization_barrier((across, peer_behind))
    pieces = [behind, across, peer_behind, swap(across)]
    wide += LANES
    dims = [(patches, wide), (patches, channels), (patches, channels), (patches, wide - channels)]
    send, inner, value, side = call(
        project_kernel,
        [shape(d, BF16) for d in dims],
        pieces + prepared[3:] + started,
        2 * 10**9,
        [pltpu.VMEM((patches, counts[1]), BF16), pltpu.VMEM((patches, LANES), F32)],
    )
    got = exchange(send)
    (back,) = call(
        column_kernel,
        [shape((patches, channels), BF16)],
        [got],
        8 * 10**8,
        [pltpu.VMEM((patches, wide), BF16), pltpu.VMEM((patches, channels), BF16)],
    )
    back = exchange(back)
    w_keep, w_give = call(
        arrange_kernel,
        [shape((channels, 4 * part), BF16)] * 2,
        [w_out],
        10**7,
        [pltpu.SemaphoreType.DMA((8,))],
        in_hbm=(0,),
    )
    w_got = swap(w_give)
    (row,) = call(
        row_kernel, [shape((patches, channels), F32)], [value, side, inner, skip_wide], 8 * 10**8
    )
    (gated,) = call(
        gate_kernel, [shape((patches, channels), BF16)], [back, row, out_gain], 4 * 10**8
    )
    operands = [gated, swap(gated), w_keep, w_got]
    (far,) = call(far_kernel, [shape((patches, part), BF16)], operands, 4 * 10**8)
    far = hop(far, 1)
    near, next_sum, mine = call(
        output_kernel,
        [shape((patches, part), BF16)] + [shape((patches, part), F32)] * 2,
        operands + [flat],
        2 * 10**9,
    )
    near = hop(near, -1)
    last = hop((next_sum + far.astype(F32)).astype(BF16), 1)
    total = mine + near.astype(F32) + last.astype(F32)
    return total.astype(BF16).reshape(tokens.shape)


def solution(mesh):
    return jax.shard_map(
        layer,
        mesh=mesh,
        in_specs=(
            P(None, "space", None, "tensor"),
            P(),
            P(None, "tensor"),
            P(),
            P(None, "tensor"),
            P("tensor"),
            P("tensor"),
            P("tensor"),
            P("tensor"),
            P("tensor", None),
        ),
        out_specs=P(None, "space", None, "tensor"),
        check_vma=False,
    )
```

```python
import jax
import jax.numpy as jnp
from jax import lax
from jax.experimental import pallas as pl
from jax.experimental.pallas import tpu as pltpu
from jax.sharding import PartitionSpec as P

HEAD_DIM = 64
STATE = 128
LANES = 128
EPS = 1e-05
BF16 = jnp.bfloat16
F32 = jnp.float32


def dot(a, b, dims=((1,), (0,))):
    return lax.dot_general(a, b, (dims, ((), ())), preferred_element_type=F32)


def one_hot(rows, cols, target):
    t = lax.broadcasted_iota(jnp.int32, (rows, 1), 0)
    q = lax.broadcasted_iota(jnp.int32, (rows, cols), 1)
    return jnp.where(target(t) == q, 1.0, 0.0).astype(BF16)


def block(chip, core, part):
    chips = 4
    offset = (((chip + 2 * chips) & (chips - 1)) * 2 + core) * part
    return pl.ds(pl.multiple_of(offset, part), part)


def position():
    place = lax.axis_index("tensor")
    core = place & 1
    return place >> 1, core, 1 - 2 * core


def spots():
    y_hi, core, way = position()
    other = 1 - core
    early = [(y_hi, core), (y_hi - way, core), (y_hi, other), (y_hi + way, other)]
    late = [(y_hi + way, core), (y_hi + 2, core), (y_hi - way, other), (y_hi + 2, other)]
    return early, late


def scaled(pieces, gain_ref, squares, y_ref, counted=0):
    step_rows = 64
    part = pieces[0].shape[1]
    gains = [gain_ref[k : k + 1, :] for k in range(len(pieces))]

    def some(n, carry):
        rows = pl.ds(pl.multiple_of(n * step_rows, step_rows), step_rows)
        total = squares(rows)
        for k, ref in enumerate(pieces):
            x = ref[rows, :].astype(F32)
            y_ref[rows, k * part : (k + 1) * part] = (x * gains[k]).astype(BF16)
            if k < counted:
                continue
            x = x * x
            for m in range(part // LANES):
                total += x[:, m * LANES : (m + 1) * LANES]
        carry[rows, :] = total

    def loop(out_ref):
        @pl.loop(0, y_ref.shape[0] // step_rows)
        def _(n):
            some(n, out_ref)

    return loop


def prepare_kernel(*refs):
    gain_ref, w_inner_hbm, w_bc_hbm, w_step_ref, bias_ref, rate_ref = refs[:6]
    outs, small_ref, sems = (refs[6:9], refs[9:12]), refs[12], refs[13]
    channels, states = w_inner_hbm.shape[1], w_bc_hbm.shape[1]
    heads = w_step_ref.shape[0]
    part = outs[0][2].shape[1]
    copies = []
    for (w_ref, step_ref, gains_ref), blocks in zip(outs, spots()):
        for k, (chip, side) in enumerate(blocks):
            for source, lanes in ((w_inner_hbm, (0, channels)), (w_bc_hbm, (channels, states))):
                copy = pltpu.make_async_copy(
                    source.at[block(chip, side, part), :],
                    w_ref.at[pl.ds(k * part, part), pl.ds(*lanes)],
                    sems.at[len(copies)],
                )
                copy.start()
                copies.append(copy)
    small_ref[...] = jnp.zeros_like(small_ref)
    small_ref[0:1, :heads] = bias_ref[...]
    small_ref[1:2, :heads] = rate_ref[...]
    for (w_ref, step_ref, gains_ref), blocks in zip(outs, spots()):
        step_ref[...] = jnp.zeros_like(step_ref)
        gains_ref[...] = jnp.zeros_like(gains_ref)
        for k, (chip, side) in enumerate(blocks):
            step_ref[:heads, k * part : (k + 1) * part] = w_step_ref[:, block(chip, side, part)]
            row = ((chip + 8) & 3) * 4 + side * 2
            for m in range(part // LANES):
                gains_ref[k : k + 1, m * LANES : (m + 1) * LANES] = gain_ref[pl.ds(row + m, 1), :]
    for copy in copies:
        copy.wait()


def squares_kernel(x_ref, squares_ref):
    x = x_ref[...].astype(F32)
    x = x * x
    squares_ref[...] = x[:, :LANES] + x[:, LANES:]


def first_kernel(*refs):
    pieces = refs[:4]
    w_ref, step_ref, gain_ref, begun_ref = refs[4:8]
    acc_ref, squares_ref, y_ref = refs[8:]
    wide = w_ref.shape[1]
    scaled(pieces, gain_ref, lambda rows: begun_ref[rows, :], y_ref, 1)(squares_ref)
    y = y_ref[...]
    acc_ref[:, :wide] = dot(y, w_ref[...])
    acc_ref[:, wide:] = dot(y, step_ref[...], ((1,), (1,)))


def gathered(x, b):
    return jnp.concatenate([x[n * 128 + b * 64 : n * 128 + b * 64 + 64] for n in range(4)], axis=0)


def project_kernel(*refs):
    pieces = refs[:4]
    w_ref, step_ref, gain_ref, small_ref, acc_ref, squares_ref = refs[4:10]
    send_ref, inner_ref, value_ref, side_ref = refs[10:14]
    y_ref, total_ref = refs[14:]
    patches = pieces[0].shape[0]
    channels = inner_ref.shape[1]
    wide = w_ref.shape[1]
    states = wide - channels
    scaled(pieces, gain_ref, lambda rows: squares_ref[rows, :], y_ref)(total_ref)
    mean = jnp.sum(total_ref[...], axis=-1, keepdims=True) / (2 * y_ref.shape[1])
    scale = lax.rsqrt(mean + EPS)
    y = y_ref[...]
    raw = acc_ref[:, wide:] + dot(y, step_ref[...], ((1,), (1,)))
    step = jax.nn.softplus(raw * scale + small_ref[0:1, :])
    side_ref[:, states:] = (-small_ref[1:2, :] * step).astype(BF16)
    maps = acc_ref[:, channels:wide] + dot(y, w_ref[:, channels:])
    side_ref[:, :states] = (maps * scale).astype(BF16)
    inner = ((acc_ref[:, :channels] + dot(y, w_ref[:, :channels])) * scale).astype(BF16)
    inner_ref[...] = inner
    left = lax.broadcasted_iota(jnp.int32, (patches, LANES), 1) < HEAD_DIM
    for k in range(channels // LANES):
        widened = jnp.where(left, step[:, 2 * k : 2 * k + 1], step[:, 2 * k + 1 : 2 * k + 2])
        at = slice(k * LANES, (k + 1) * LANES)
        value_ref[:, at] = (inner[:, at].astype(F32) * widened).astype(BF16)
    target = lambda t: ((t & 3) << 6) + ((t >> 3) << 1) + ((t >> 2) & 1)
    order = one_hot(256, 256, target)
    for b in range(patches // 256):
        rows = slice(b * 256, (b + 1) * 256)
        send_ref[rows, :channels] = dot(order, gathered(value_ref, b)).astype(BF16)
        send_ref[rows, channels:] = dot(order, gathered(side_ref, b)).astype(BF16)


def scan(value, side):
    length = value.shape[0]
    heads = value.shape[1] // HEAD_DIM
    in_map, out_map = side[:, :STATE], side[:, STATE : 2 * STATE]
    decay = side[:, 2 * STATE :]
    scores = dot(out_map, in_map, ((1,), (1,)))
    t = lax.broadcasted_iota(jnp.int32, (length, length), 0)
    r = lax.broadcasted_iota(jnp.int32, (length, length), 1)
    lower = jnp.where(t >= r, 1.0, 0.0).astype(BF16)
    upper = jnp.where(t <= r, 1.0, 0.0).astype(BF16)
    unit = jnp.where(t == r, 1.0, 0.0).astype(BF16)
    running = dot(lower, decay)
    across = dot(decay, upper, ((0,), (0,)))
    shifted = running - decay.astype(F32)
    shifted_across = across - dot(decay, unit, ((0,), (0,)))
    doubled = jnp.where(t == r, 2.0 * scores, scores)
    below = r < t
    left = lax.broadcasted_iota(jnp.int32, (length, LANES), 1) < HEAD_DIM

    def weights(h):
        later = running[:, h : h + 1] - across[h : h + 1, :]
        earlier = shifted_across[h : h + 1, :] - shifted[:, h : h + 1]
        return (doubled * jnp.exp(jnp.where(below, later, earlier))).astype(BF16)

    outs = []
    for k in range(heads // 2):
        pair = value[:, k * LANES : (k + 1) * LANES]
        zero = jnp.zeros_like(pair)
        stacked = jnp.concatenate([jnp.where(left, pair, zero), jnp.where(left, zero, pair)], axis=0)
        both = jnp.concatenate([weights(2 * k), weights(2 * k + 1)], axis=1)
        outs.append(dot(both, stacked))
    return jnp.concatenate(outs, axis=1)


def row_kernel(value_ref, side_ref, inner_ref, skip_ref, out_ref):
    length = LANES
    left = lax.broadcasted_iota(jnp.int32, (1, LANES), 1) < HEAD_DIM
    heads = skip_ref.shape[1]
    skip = jnp.concatenate(
        [
            jnp.where(left, skip_ref[0:1, k : k + 1], skip_ref[0:1, k + 1 : k + 2])
            for k in range(0, heads, 2)
        ],
        axis=1,
    )
    for row in range(value_ref.shape[0] // length):
        at = pl.ds(row * length, length)
        out_ref[at, :] = (
            scan(value_ref[at, :], side_ref[at, :]) + skip * inner_ref[at, :].astype(F32)
        )


def column_kernel(recv_ref, back_ref, sorted_ref, outs_ref):
    rows = recv_ref.shape[0]
    channels = back_ref.shape[1]
    length = rows // 4
    order = one_hot(256, 256, lambda t: (((t & 63) >> 1) << 3) + ((t >> 6) << 1) + (t & 1))
    for b in range(rows // 256):
        block_rows = dot(order, recv_ref[b * 256 : (b + 1) * 256, :]).astype(BF16)
        for n in range(4):
            sorted_ref[n * length + b * 64 : n * length + b * 64 + 64, :] = block_rows[n * 64 : n * 64 + 64]
    for n in range(4):
        at = pl.ds(n * length, length)
        outs_ref[at, :] = scan(sorted_ref[at, :channels], sorted_ref[at, channels:]).astype(BF16)
    back = one_hot(256, 256, lambda t: (((t >> 1) & 3) << 6) + ((t >> 3) << 1) + (t & 1))
    for b in range(rows // 256):
        back_ref[b * 256 : (b + 1) * 256, :] = dot(back, gathered(outs_ref, b)).astype(BF16)


def arrange_kernel(w_hbm, keep_ref, give_ref, sems):
    y_hi, core, way = position()
    part = keep_ref.shape[1] // 4
    copies = []
    for ref, side, toward in ((give_ref, 1 - core, -way), (keep_ref, core, way)):
        for k, chip in enumerate((2, -toward, toward, 0)):
            copy = pltpu.make_async_copy(
                w_hbm.at[:, block(y_hi + chip, side, part)],
                ref.at[:, pl.ds(k * part, part)],
                sems.at[len(copies)],
            )
            copy.start()
            copies.append(copy)
    for copy in copies:
        copy.wait()


def gate_kernel(back_ref, row_ref, gain_ref, gated_ref):
    order = one_hot(256, 256, lambda t: (((t & 63) >> 1) << 3) + ((t & 1) << 2) + (t >> 6))
    gain = jnp.concatenate([gain_ref[k : k + 1, :] for k in range(gain_ref.shape[0])], axis=1)
    for b in range(row_ref.shape[0] // 256):
        total = gathered(row_ref, b) + dot(order, back_ref[b * 256 : (b + 1) * 256, :])
        scale = lax.rsqrt(jnp.mean(total * total, axis=-1, keepdims=True) + EPS)
        gated = (total * scale * gain).astype(BF16)
        for n in range(4):
            gated_ref[n * 128 + b * 64 : n * 128 + b * 64 + 64, :] = gated[n * 64 : n * 64 + 64]


def far_kernel(gated_ref, peer_ref, keep_ref, got_ref, far_ref):
    at = slice(0, far_ref.shape[1])
    far_ref[...] = (
        dot(gated_ref[...], keep_ref[:, at]) + dot(peer_ref[...], got_ref[:, at])
    ).astype(BF16)


def output_kernel(gated_ref, peer_ref, keep_ref, got_ref, tokens_ref, near_ref, last_ref, own_ref):
    part = near_ref.shape[1]
    gated, peer = gated_ref[...], peer_ref[...]
    for k, ref in enumerate((near_ref, last_ref, own_ref)):
        at = slice((k + 1) * part, (k + 2) * part)
        total = dot(gated, keep_ref[:, at]) + dot(peer, got_ref[:, at])
        if ref is own_ref:
            total += tokens_ref[...]
        ref[...] = total.astype(ref.dtype)


def call(body, outs, args, flops, scratch=(), in_hbm=()):
    size = sum(a.size * a.dtype.itemsize for a in args)
    size += sum(o.size * o.dtype.itemsize for o in outs)
    return pl.pallas_call(
        body,
        out_shape=outs,
        in_specs=[
            pl.BlockSpec(memory_space=pltpu.HBM if n in in_hbm else pltpu.VMEM)
            for n in range(len(args))
        ],
        out_specs=[pl.BlockSpec(memory_space=pltpu.VMEM)] * len(outs),
        scratch_shapes=list(scratch),
        cost_estimate=pl.CostEstimate(flops=flops, bytes_accessed=size, transcendentals=0),
        compiler_params=pltpu.CompilerParams(vmem_limit_bytes=24 * 1024 * 1024),
    )(*args)


def shape(dims, dtype):
    return jax.ShapeDtypeStruct(dims, dtype)


def hop(x, sign):
    pairs = []
    for t in range(8):
        way = sign * (1 - 2 * (t & 1))
        pairs.append((t, (t + 2 * way) % 8))
    return lax.ppermute(x, "tensor", pairs)


def swap(x):
    return lax.ppermute(x, "tensor", [(t, t ^ 1) for t in range(8)])


def layer(
    tokens, in_gain, w_inner, w_bc, w_step, step_bias, decay_rate, skip, norm_gain, w_out
):
    images, rows, width, part = tokens.shape
    patches = images * rows * width
    channels = w_inner.shape[1]
    gain = in_gain.reshape(-1, LANES)
    bias = step_bias[None, :]
    rate = decay_rate[None, :]
    out_gain = norm_gain.reshape(-1, LANES)
    flat = tokens.reshape(patches, part)
    space = lax.axis_size("space")

    def exchange(x):
        y = x.reshape(space, -1, x.shape[-1])
        y = lax.all_to_all(y, "space", split_axis=0, concat_axis=0, tiled=True)
        return y.reshape(x.shape)

    x = flat.astype(BF16)
    ahead, behind = hop(x, 1), hop(x, -1)
    wide = channels + 2 * STATE
    counts = [4 * part, 4 * part]
    orders = [
        o
        for n in counts
        for o in (shape((n, wide), BF16), shape((LANES, n), BF16), shape((8, part), F32))
    ]
    (begun,) = call(squares_kernel, [shape((patches, LANES), F32)], [x], 4 * 10**10)
    begun, *sources = lax.optimization_barrier((begun, gain, w_inner, w_bc, w_step.T, bias, rate))
    prepared = call(
        prepare_kernel,
        orders + [shape((8, LANES), F32)],
        sources,
        4 * 10**9,
        [pltpu.SemaphoreType.DMA((16,))],
        in_hbm=(1, 2),
    )
    ahead, *prepared = lax.optimization_barrier((ahead, *prepared))
    across = hop(ahead, 1)
    early = [x, ahead, swap(x), swap(ahead)]
    started = call(
        first_kernel,
        [shape((patches, wide + LANES), F32), shape((patches, LANES), F32)],
        early + prepared[:3] + [begun],
        4 * 10**9,
        [pltpu.VMEM((patches, counts[0]), BF16)],
    )
    peer_behind = swap(behind)
    across, peer_behind, *started = lax.optimization_barrier((across, peer_behind, *started))
    pieces = [behind, across, peer_behind, swap(across)]
    wide += LANES
    dims = [(patches, wide), (patches, channels), (patches, channels), (patches, wide - channels)]
    send, inner, value, side = call(
        project_kernel,
        [shape(d, BF16) for d in dims],
        pieces + prepared[3:] + started,
        2 * 10**9,
        [pltpu.VMEM((patches, counts[1]), BF16), pltpu.VMEM((patches, LANES), F32)],
    )
    got = exchange(send)
    (back,) = call(
        column_kernel,
        [shape((patches, channels), BF16)],
        [got],
        8 * 10**8,
        [pltpu.VMEM((patches, wide), BF16), pltpu.VMEM((patches, channels), BF16)],
    )
    back = exchange(back)
    w_keep, w_give = call(
        arrange_kernel,
        [shape((channels, 4 * part), BF16)] * 2,
        [w_out],
        10**7,
        [pltpu.SemaphoreType.DMA((8,))],
        in_hbm=(0,),
    )
    w_got = swap(w_give)
    (row,) = call(
        row_kernel, [shape((patches, channels), F32)], [value, side, inner, skip[None, :]], 8 * 10**8
    )
    (gated,) = call(
        gate_kernel, [shape((patches, channels), BF16)], [back, row, out_gain], 4 * 10**8
    )
    operands = [gated, swap(gated), w_keep, w_got]
    (far,) = call(far_kernel, [shape((patches, part), BF16)], operands, 4 * 10**8)
    far = hop(far, 1)
    near, next_sum, mine = call(
        output_kernel,
        [shape((patches, part), BF16)] + [shape((patches, part), F32)] * 2,
        operands + [flat],
        2 * 10**9,
    )
    near = hop(near, -1)
    last = hop((next_sum + far.astype(F32)).astype(BF16), 1)
    total = mine + near.astype(F32) + last.astype(F32)
    return total.astype(BF16).reshape(tokens.shape)


def solution(mesh):
    return jax.shard_map(
        layer,
        mesh=mesh,
        in_specs=(
            P(None, "space", None, "tensor"),
            P(),
            P(None, "tensor"),
            P(),
            P(None, "tensor"),
            P("tensor"),
            P("tensor"),
            P("tensor"),
            P("tensor"),
            P("tensor", None),
        ),
        out_specs=P(None, "space", None, "tensor"),
        check_vma=False,
    )
```
